32 devices in a mesh: pipe: 4 (over z), tensor: 4 (over x, core), dp: 2 (over y).
Axes of the slice: x: 2, y: 2, z: 4, core: 2. Of those that a mesh axis runs over, the one named last changes fastest.
Arguments:
- hidden: bfloat16 [256, 4608], P(('pipe', 'dp'), 'tensor'), may hold values from -12 to 12
- weight: bfloat16 [131072, 4608], P(('pipe', 'tensor', 'dp')), may hold values from -0.5 to 0.5
- targets: int32 [256], P(('pipe', 'dp')), may hold values from 0 to 131071
- loss_grad: bfloat16 [256], P(('pipe', 'dp')), may hold values from 2 to 20
Outputs:
- token_loss: float32 [256], P(('pipe', 'dp'))
- weight_grad: bfloat16 [131072, 4608], P(('pipe', 'tensor', 'dp'))
- input_grad: bfloat16 [256, 4608], P(('pipe', 'dp'), 'tensor')
The draws below stay inside these ranges and needn't reach their ends.
All inputs are finite; a program needn't handle non-finite values.
Results may differ from the reference program's by a relative error of at most 0.017.
Values may be sent and summed in bfloat16 or wider, within the bound.
No kernel may reach another device: no remote copies, remote signals or barrier semaphores. Data moves between devices by JAX's collectives and lax.ppermute only.
A program may use at most 256 MiB of HBM per device.

```python
import math
import jax
import jax.numpy as jnp
import numpy as np
from jax import lax

D = 4608
VOCAB = 131072
TOK_DEV = 32
TOKENS = 256
N_PIPE = 4
N_DP = 2


def joint_draw(key):
    base_key = jax.random.fold_in(key, 31)
    key_rows, key_weight = jax.random.split(base_key, 2)
    weight_scale = 3.0 / math.sqrt(D)
    weight = jax.random.normal(key_weight, (VOCAB, D), jnp.float32) * weight_scale
    hidden = jax.random.normal(key_rows, (TOKENS, D), jnp.float32)
    return (jnp.clip(hidden, -12.0, 12.0), jnp.clip(weight, -0.5, 0.5))


def draw_hidden(key, part):
    return joint_draw(key)[0].astype(jnp.bfloat16)


def draw_weight(key, part):
    return joint_draw(key)[1].astype(jnp.bfloat16)


def set_ends(result, rng, least, top_value):
    longest = result.shape.index(max(result.shape))
    spots = []
    for shift in (0, 1):
        where = [jax.random.randint(jax.random.fold_in(rng, axis), (), 0, length) for axis, length in enumerate(result.shape)]
        where[longest] = (where[longest] + shift) % result.shape[longest]
        spots.append(tuple(where))
    return result.at[spots[0]].set(least).at[spots[1]].set(top_value)


def level_of(own_key, extent, shards, least, high):
    factor_of, own = 1.0, jax.random.fold_in(own_key, 6)
    for position, blocks in shards:
        draws = jnp.exp(jax.random.uniform(jax.random.fold_in(own, position), (blocks,), jnp.float32, least / len(shards), high / len(shards)))
        factor_of = factor_of * jnp.repeat(draws, extent[position] // blocks).reshape([-1 if axis == position else 1 for axis in range(len(extent))])
    return factor_of


def ranked_wide(own_key, dims, amount, skew):
    portions = [min(1 << octave, amount + 1 - (1 << octave)) * (1 << 20) // math.isqrt((1 << octave) ** skew) + 1 for octave in range((amount + 1).bit_length()) if 1 << octave <= amount]
    spread = 1 + sum(portions) // (1 << 30)
    listing = np.cumsum(np.array([max(1, weight // spread) for weight in portions]))
    lot = jax.random.randint(jax.random.fold_in(own_key, 1), dims, 0, int(listing[len(portions) - 1]))
    start = jnp.left_shift(1, jnp.searchsorted(jnp.asarray(listing, jnp.int32), lot, side="right").astype(jnp.int32))
    rank = start - 1 + jax.random.randint(jax.random.fold_in(own_key, 4), dims, 0, 1 << 30) % jnp.minimum(start, amount + 1 - start)
    return jax.random.permutation(jax.random.fold_in(own_key, 2), amount)[rank].astype(jnp.int32)


def setup_inputs(seed: int = 0) -> dict:
    arg_keys = jax.random.split(jax.random.key(seed), 5)
    hidden = draw_hidden(jax.random.fold_in(arg_keys[4], 71), 0)
    weight = draw_weight(jax.random.fold_in(arg_keys[4], 71), 0)
    targets = set_ends(ranked_wide(arg_keys[2], (TOKENS,), VOCAB, 2), jax.random.fold_in(arg_keys[2], 3), 0, VOCAB - 1).astype(jnp.int32)
    loss_grad = jnp.clip(jnp.exp(math.log(20.0) - 2.3025851 * jax.random.uniform(arg_keys[3], (TOKENS,), jnp.float32) ** level_of(arg_keys[3], (TOKENS,), ((0, 8),), -0.2, 0.2)), 2.0, 20.0).astype(jnp.bfloat16)
    return dict(hidden=hidden, weight=weight, targets=targets, loss_grad=loss_grad)


def by_replica(values):
    shaped = values.reshape((N_PIPE, N_DP, TOK_DEV) + values.shape[1:])
    return jnp.moveaxis(shaped, 1, 0).reshape((N_DP, N_PIPE * TOK_DEV) + values.shape[1:])


def back_order(values):
    shaped = values.reshape((N_DP, N_PIPE, TOK_DEV) + values.shape[2:])
    return jnp.moveaxis(shaped, 0, 1).reshape((N_DP * N_PIPE * TOK_DEV,) + values.shape[2:])


def reference(hidden, weight, targets, loss_grad):
    rows_all = by_replica(hidden)
    grads_all = by_replica(loss_grad)
    target_all = by_replica(targets)
    vocab_ids = lax.broadcasted_iota(jnp.int32, (1, weight.shape[0]), 1)
    losses = []
    input_grads = []
    summed = None
    for replica in range(N_DP):
        rows = rows_all[replica]
        logits = jnp.dot(rows, weight.T, preferred_element_type=jnp.float32)
        onehot = (vocab_ids == target_all[replica].astype(jnp.int32)[:, None]).astype(jnp.float32)
        row_top = jnp.max(logits, axis=1)
        logsum = row_top + jnp.log(jnp.sum(jnp.exp(logits - row_top[:, None]), axis=1))
        picked = jnp.sum(logits * onehot, axis=1)
        losses.append(logsum - picked)
        scale = grads_all[replica].astype(jnp.float32)[:, None]
        grad_logits = (scale * (jnp.exp(logits - logsum[:, None]) - onehot)).astype(jnp.bfloat16)
        input_grads.append(jnp.dot(grad_logits, weight, preferred_element_type=jnp.float32).astype(jnp.bfloat16))
        partial_grad = lax.dot_general(grad_logits, rows, (((0,), (0,)), ((), ())), preferred_element_type=jnp.float32)
        partial_grad = lax.optimization_barrier(partial_grad.astype(jnp.bfloat16)).astype(jnp.float32)
        summed = partial_grad if summed is None else summed + partial_grad
    weight_grad = summed.astype(jnp.bfloat16)
    return back_order(jnp.stack(losses)), weight_grad, back_order(jnp.stack(input_grads))
```

```python
import functools

import jax
import jax.numpy as jnp
from jax import lax
from jax.experimental import pallas as pl
from jax.experimental.pallas import tpu as pltpu
from jax.sharding import PartitionSpec as P

AXES = ("pipe", "tensor", "dp")
VMEM = 56 * 1024 * 1024


def params(**kw):
    return pltpu.CompilerParams(vmem_limit_bytes=VMEM, **kw)


def whole(shape):
    return pl.BlockSpec(shape, lambda *a: (0,) * len(shape))


class Grid:
    def __init__(self, sizes):
        self.pipe, self.tensor, self.dp = sizes

    def perm(self, move):
        pairs = []
        for z in range(self.pipe):
            for t in range(self.tensor):
                for y in range(self.dp):
                    source = (z * self.tensor + t) * self.dp + y
                    z2, x2, c2, y2 = move(z, t // 2, t % 2, y)
                    pairs.append((source, (z2 * self.tensor + 2 * x2 + c2) * self.dp + y2))
        return pairs

    def send(self, value, move):
        return lax.ppermute(value, AXES, self.perm(move))


def core_swap(z, x, c, y):
    return z, x, 1 - c, y


def first_swap(z, x, c, y):
    return (z, 1 - x, c, y) if c == 0 else (z, x, c, 1 - y)


def second_swap(z, x, c, y):
    return (z, x, c, 1 - y) if c == 0 else (z, 1 - x, c, y)


def x_swap(z, x, c, y):
    return z, 1 - x, c, y


def y_swap(z, x, c, y):
    return z, x, c, 1 - y


def z_swap(k):
    return lambda z, x, c, y: (z ^ k, x, c, y)


def logits_kernel(place, ids, *refs, pieces, tok, width):
    parts, (w, h, lt, stats) = refs[:pieces], refs[pieces:]
    step = pl.program_id(0)
    rows = w.shape[0]

    @pl.when(step == 0)
    def _():
        for n, part in enumerate(parts):
            for k in range(part.shape[0]):
                at = n * part.shape[0] + k
                row = pl.multiple_of(place[0, at] * tok, tok)
                col = pl.multiple_of(place[1, at] * width, 128)
                h[pl.ds(row, tok), pl.ds(col, width)] = part[k]
        stats[...] = jnp.zeros_like(stats)
        stats[0:1, :] = jnp.full_like(stats[0:1, :], -jnp.inf)

    value = lax.dot_general(
        w[...], h[...], (((1,), (1,)), ((), ())), preferred_element_type=jnp.float32
    )
    lt[...] = value
    top = stats[0:1, :]
    new_top = jnp.maximum(top, jnp.max(value, axis=0, keepdims=True))
    stats[0:1, :] = new_top
    stats[1:2, :] = stats[1:2, :] * jnp.exp(top - new_top) + jnp.sum(
        jnp.exp(value - new_top), axis=0, keepdims=True
    )
    index = lax.broadcasted_iota(jnp.int32, value.shape, 0) + step * rows
    stats[2:3, :] += jnp.sum(jnp.where(index == ids[...], value, 0.0), axis=0, keepdims=True)


def logits_call(place, ids, parts, weight, tokens, block):
    vocab, wide = weight.shape
    tok, width = parts[0].shape[1:]
    body = functools.partial(logits_kernel, pieces=len(parts), tok=tok, width=width)
    return pl.pallas_call(
        body,
        grid_spec=pltpu.PrefetchScalarGridSpec(
            num_scalar_prefetch=1,
            grid=(vocab // block,),
            in_specs=[whole((1, tokens))]
            + [whole(part.shape) for part in parts]
            + [pl.BlockSpec((block, wide), lambda i, *_: (i, 0))],
            out_specs=[
                whole((tokens, wide)),
                pl.BlockSpec((block, tokens), lambda i, *_: (i, 0)),
                whole((8, tokens)),
            ],
        ),
        out_shape=[
            jax.ShapeDtypeStruct((tokens, wide), jnp.bfloat16),
            jax.ShapeDtypeStruct((vocab, tokens), jnp.float32),
            jax.ShapeDtypeStruct((8, tokens), jnp.float32),
        ],
        compiler_params=params(),
        cost_estimate=pl.CostEstimate(
            flops=2 * vocab * wide * tokens, bytes_accessed=2 * vocab * wide, transcendentals=0
        ),
        name="logits",
    )(place, ids, *parts, weight)


def input_kernel(place, ids, logsum, scale, lt, w, gt, keep, away, acc, *, tok, width):
    step = pl.program_id(0)
    rows = lt.shape[0]
    index = lax.broadcasted_iota(jnp.int32, lt.shape, 0) + step * rows
    hot = jnp.where(index == ids[...], 1.0, 0.0)
    grad = (scale[...] * (jnp.exp(lt[...] - logsum[...]) - hot)).astype(jnp.bfloat16)
    gt[...] = grad
    term = lax.dot_general(
        grad, w[...], (((0,), (0,)), ((), ())), preferred_element_type=jnp.float32
    )

    @pl.when(step == 0)
    def _():
        acc[...] = term

    @pl.when(step > 0)
    def _():
        acc[...] += term

    @pl.when(step == pl.num_programs(0) - 1)
    def _():
        half = keep.shape[0]
        for at in range(2 * half):
            row = pl.multiple_of(place[0, at] * tok, tok)
            col = pl.multiple_of(place[1, at] * width, 128)
            out = keep if at < half else away
            out[at % half] = acc[pl.ds(row, tok), pl.ds(col, width)].astype(jnp.bfloat16)


def input_call(place, ids, logsum, scale, lt, weight, tok, width, block):
    vocab, wide = weight.shape
    tokens = lt.shape[1]
    half = (tokens // tok) * (wide // width) // 2
    return pl.pallas_call(
        functools.partial(input_kernel, tok=tok, width=width),
        grid_spec=pltpu.PrefetchScalarGridSpec(
            num_scalar_prefetch=1,
            grid=(vocab // block,),
            in_specs=[
                whole((1, tokens)),
                whole((1, tokens)),
                whole((1, tokens)),
                pl.BlockSpec((block, tokens), lambda i, *_: (i, 0)),
                pl.BlockSpec((block, wide), lambda i, *_: (i, 0)),
            ],
            out_specs=[
                pl.BlockSpec((block, tokens), lambda i, *_: (i, 0)),
                whole((half, tok, width)),
                whole((half, tok, width)),
            ],
            scratch_shapes=[pltpu.VMEM((tokens, wide), jnp.float32)],
        ),
        out_shape=[
            jax.ShapeDtypeStruct((vocab, tokens), jnp.bfloat16),
            jax.ShapeDtypeStruct((half, tok, width), jnp.bfloat16),
            jax.ShapeDtypeStruct((half, tok, width), jnp.bfloat16),
        ],
        compiler_params=params(),
        cost_estimate=pl.CostEstimate(
            flops=2 * vocab * wide * tokens, bytes_accessed=2 * vocab * wide, transcendentals=0
        ),
        name="input_grad",
    )(place, ids, logsum, scale, lt, weight)


def weight_kernel(gt, h, out):
    out[...] = jnp.dot(gt[...], h[...], preferred_element_type=jnp.float32).astype(jnp.bfloat16)


def weight_call(gt, h, block):
    vocab, tokens = gt.shape
    wide = h.shape[1]
    return pl.pallas_call(
        weight_kernel,
        grid=(vocab // block,),
        in_specs=[pl.BlockSpec((block, tokens), lambda i: (i, 0)), whole((tokens, wide))],
        out_specs=pl.BlockSpec((block, wide), lambda i: (i, 0)),
        out_shape=jax.ShapeDtypeStruct((vocab, wide), jnp.bfloat16),
        compiler_params=params(),
        cost_estimate=pl.CostEstimate(
            flops=2 * vocab * wide * tokens, bytes_accessed=2 * vocab * wide, transcendentals=0
        ),
        name="weight_grad",
    )(gt, h)


def merge(a, b):
    top = jnp.maximum(a[0], b[0])
    total = a[1] * jnp.exp(a[0] - top) + b[1] * jnp.exp(b[0] - top)
    return jnp.stack([top, total, a[2] + b[2]])


def places(grid):
    z, t, y = (lax.axis_index(name) for name in AXES)
    x, c = t // 2, t % 2
    rows, cols = [], []
    for dc in range(2):
        core = c ^ dc
        for dz in range(grid.pipe):
            for b2 in range(2):
                for b1 in range(2):
                    dx = jnp.where(core == 0, b1, b2)
                    dy = jnp.where(core == 0, b2, b1)
                    rows.append((z ^ dz) * grid.dp + (y ^ dy))
                    cols.append(2 * (x ^ dx) + core)
    return jnp.stack([jnp.stack(rows), jnp.stack(cols)]).astype(jnp.int32)


def gather_fast(grid, hidden):
    mine, theirs = [], []
    for dz in range(grid.pipe):
        own = hidden if dz == 0 else grid.send(hidden, z_swap(dz))
        first = grid.send(own, first_swap)
        second = grid.send(own, second_swap)
        both = grid.send(first, second_swap)
        mine.append(jnp.stack([own, first, second, both]))
    for part in mine:
        theirs.append(grid.send(part, core_swap))
    return mine + theirs


def gather_rows(grid, value):
    parts = [value if dz == 0 else grid.send(value, z_swap(dz)) for dz in range(grid.pipe)]
    held = jnp.stack(parts)
    held = jnp.stack([held, grid.send(held, y_swap)], axis=1)
    z, y = lax.axis_index("pipe"), lax.axis_index("dp")
    order = [jnp.arange(grid.pipe) ^ z, jnp.arange(grid.dp) ^ y]
    held = held[order[0]][:, order[1]]
    return jnp.moveaxis(held, 2, 0).reshape(value.shape[0], -1)


def merge_fast(grid, stats):
    moves = [core_swap, x_swap, y_swap]
    k = 1
    while k < grid.pipe:
        moves.append(z_swap(k))
        k *= 2
    for move in moves:
        stats = merge(stats, grid.send(stats, move))
    return stats


def plus(*terms):
    return sum(term.astype(jnp.float32) for term in terms).astype(jnp.bfloat16)


def scatter_fast(grid, keep, away):
    shape = (grid.pipe, 2, 2) + keep.shape[1:]
    held = plus(keep, grid.send(away, core_swap)).reshape(shape)
    held = plus(held[:, 0], grid.send(held[:, 1], second_swap))
    held = plus(held[:, 0], grid.send(held[:, 1], first_swap))
    return plus(held[0], *[grid.send(held[k], z_swap(k)) for k in range(1, grid.pipe)])


def local(grid, hidden, weight, targets, loss_grad):
    tok, width = hidden.shape
    vocab, wide = weight.shape
    tokens = tok * grid.pipe * grid.dp
    z, t, y = (lax.axis_index(name) for name in AXES)
    offset = ((z * grid.tensor + t) * grid.dp + y) * vocab
    block = min(512, vocab)
    fast = grid.tensor == 4 and grid.dp == 2 and grid.pipe in (1, 2, 4) and width % 128 == 0
    if fast:
        place = places(grid)
        parts = gather_fast(grid, hidden)
        ids = gather_rows(grid, targets[None])
        scale = gather_rows(grid, loss_grad[None].astype(jnp.float32))
    else:
        part = lax.all_gather(hidden, "tensor", axis=1, tiled=True)
        parts = [lax.all_gather(part, ("pipe", "dp"), axis=0)]
        count = grid.pipe * grid.dp
        place = jnp.stack([jnp.arange(count), jnp.zeros(count, jnp.int32)]).astype(jnp.int32)
        ids = lax.all_gather(targets, ("pipe", "dp"), axis=0, tiled=True)[None]
        scale = lax.all_gather(loss_grad.astype(jnp.float32), ("pipe", "dp"), axis=0, tiled=True)
        scale = scale[None]
    ids = ids - offset
    h, lt, stats = logits_call(place, ids, parts, weight, tokens, block)
    stats = stats[:3]
    if fast:
        stats = merge_fast(grid, stats)
    else:
        every = lax.all_gather(stats, AXES, axis=0)
        stats = functools.reduce(merge, [every[i] for i in range(every.shape[0])])
    logsum = stats[0:1] + jnp.log(stats[1:2])
    losses = (logsum - stats[2:3])[0]
    token_loss = lax.dynamic_slice_in_dim(losses, (z * grid.dp + y) * tok, tok, 0)
    if fast:
        gt, keep, away = input_call(place, ids, logsum, scale, lt, weight, tok, width, block)
        weight_grad = weight_call(gt, h, block)
        input_grad = scatter_fast(grid, keep, away)
    else:
        both = tokens // 2
        place = jnp.stack([jnp.arange(2), jnp.zeros(2, jnp.int32)]).astype(jnp.int32)
        gt, keep, away = input_call(place, ids, logsum, scale, lt, weight, both, wide, block)
        weight_grad = weight_call(gt, h, block)
        term = jnp.concatenate([keep[0], away[0]])
        narrowed = lax.psum_scatter(term, "tensor", scatter_dimension=1, tiled=True)
        input_grad = lax.psum_scatter(narrowed, ("pipe", "dp"), scatter_dimension=0, tiled=True)
    return token_loss, weight_grad, input_grad


def solution(mesh):
    in_specs = (
        P(("pipe", "dp"), "tensor"),
        P(("pipe", "tensor", "dp"), None),
        P(("pipe", "dp")),
        P(("pipe", "dp")),
    )
    out_specs = (P(("pipe", "dp")), P(("pipe", "tensor", "dp"), None), P(("pipe", "dp"), "tensor"))
    grid = Grid(tuple(mesh.shape[name] for name in AXES))
    return jax.shard_map(
        functools.partial(local, grid),
        mesh=mesh,
        in_specs=in_specs,
        out_specs=out_specs,
        check_vma=False,
    )
```

```python
import functools

import jax
import jax.numpy as jnp
from jax import lax
from jax.experimental import pallas as pl
from jax.experimental.pallas import tpu as pltpu
from jax.sharding import PartitionSpec as P

AXES = ("pipe", "tensor", "dp")
MIB = 1024 * 1024
INSIDE = pl.BlockSpec(memory_space=pltpu.VMEM)
SCALARS = pl.BlockSpec(memory_space=pltpu.SMEM)


def params(need):
    return pltpu.CompilerParams(vmem_limit_bytes=min(need, 58 * MIB))


def cost(vocab, wide, tokens):
    return pl.CostEstimate(
        flops=2 * vocab * wide * tokens, bytes_accessed=2 * vocab * wide, transcendentals=0
    )


def whole(shape):
    return pl.BlockSpec(shape, lambda *a: (0,) * len(shape))


class Grid:
    def __init__(self, sizes):
        self.pipe, self.tensor, self.dp = sizes

    def perm(self, move):
        pairs = []
        for z in range(self.pipe):
            for t in range(self.tensor):
                for y in range(self.dp):
                    source = (z * self.tensor + t) * self.dp + y
                    z2, x2, c2, y2 = move(z, t // 2, t % 2, y)
                    pairs.append((source, (z2 * self.tensor + 2 * x2 + c2) * self.dp + y2))
        return pairs

    def send(self, value, move):
        return lax.ppermute(value, AXES, self.perm(move))


def core_swap(z, x, c, y):
    return z, x, 1 - c, y


def first_swap(z, x, c, y):
    return (z, 1 - x, c, y) if c == 0 else (z, x, c, 1 - y)


def second_swap(z, x, c, y):
    return (z, x, c, 1 - y) if c == 0 else (z, 1 - x, c, y)


def x_swap(z, x, c, y):
    return z, 1 - x, c, y


def y_swap(z, x, c, y):
    return z, x, c, 1 - y


def z_swap(k):
    return lambda z, x, c, y: (z ^ k, x, c, y)


def logits_kernel(place, ids, *refs, pieces, slabs, tok, width, block):
    parts, weights = refs[:pieces], refs[pieces : pieces + slabs]
    h, lt, stats = refs[pieces + slabs :]
    for n, part in enumerate(parts):
        for k in range(part.shape[0]):
            at = n * part.shape[0] + k
            row = pl.multiple_of(place[0, at] * tok, tok)
            col = pl.multiple_of(place[1, at] * width, 128)
            h[pl.ds(row, tok), pl.ds(col, width)] = part[k]
    row = lax.broadcasted_iota(jnp.int32, stats.shape, 0)
    stats[...] = jnp.where(row == 0, -jnp.inf, 0.0)

    def multiply(step, w, row):
        rows = pl.ds(pl.multiple_of(step * block, block), block)
        lt[rows, :] = lax.dot_general(
            w[pl.ds(row, block), :],
            h[...],
            (((1,), (1,)), ((), ())),
            preferred_element_type=jnp.float32,
        )

    def collect(step):
        value = lt[pl.ds(pl.multiple_of(step * block, block), block), :]
        top = stats[0:1, :]
        new_top = jnp.maximum(top, jnp.max(value, axis=0, keepdims=True))
        stats[0:1, :] = new_top
        stats[1:2, :] = stats[1:2, :] * jnp.exp(top - new_top) + jnp.sum(
            jnp.exp(value - new_top), axis=0, keepdims=True
        )
        index = lax.broadcasted_iota(jnp.int32, value.shape, 0) + step * block
        hit = jnp.where(index == ids[...], value, 0.0)
        stats[2:3, :] += jnp.sum(hit, axis=0, keepdims=True)

    done = 0
    for w in weights:
        steps = w.shape[0] // block
        multiply(done, w, 0)
        if done:
            collect(done - 1)

        @pl.loop(1, steps)
        def _(step, w=w, done=done):
            multiply(done + step, w, pl.multiple_of(step * block, block))
            collect(done + step - 1)

        done += steps
    collect(done - 1)


def logits_call(place, ids, parts, weights, tokens, block):
    vocab, wide = sum(w.shape[0] for w in weights), weights[0].shape[1]
    tok, width = parts[0].shape[1:]
    body = functools.partial(
        logits_kernel,
        pieces=len(parts),
        slabs=len(weights),
        tok=tok,
        width=width,
        block=block,
    )
    return pl.pallas_call(
        body,
        in_specs=[SCALARS] + [INSIDE] * (len(parts) + len(weights) + 1),
        out_specs=[INSIDE] * 3,
        out_shape=[
            pltpu.VMEM((tokens, wide), jnp.bfloat16),
            pltpu.VMEM((vocab, tokens), jnp.float32),
            jax.ShapeDtypeStruct((3, tokens), jnp.float32),
        ],
        compiler_params=params(2 * MIB + 4 * block * tokens),
        cost_estimate=cost(vocab, wide, tokens),
        name="logits",
    )(place, ids, *parts, *weights)


def load_kernel(source, held, sem, *, first):
    copy = pltpu.make_async_copy(source.at[pl.ds(first, held.shape[0])], held, sem)
    copy.start()
    copy.wait()


def load_call(weight, first, count):
    return pl.pallas_call(
        functools.partial(load_kernel, first=first),
        in_specs=[pl.BlockSpec(memory_space=pltpu.HBM)],
        out_specs=INSIDE,
        out_shape=pltpu.VMEM((count, weight.shape[1]), weight.dtype),
        scratch_shapes=[pltpu.SemaphoreType.DMA],
        compiler_params=params(MIB),
        cost_estimate=cost(count, weight.shape[1], 128),
        name="load_weight",
    )(weight)


def grad_kernel(ids, rows_in, stats, lt, gt, *, block):
    scale = rows_in[1:2, :]
    logsum = stats[0:1, :] + jnp.log(stats[1:2, :])

    @pl.loop(0, lt.shape[0] // block)
    def _(step):
        rows = pl.ds(pl.multiple_of(step * block, block), block)
        index = lax.broadcasted_iota(jnp.int32, (block, lt.shape[1]), 0) + step * block
        hot = jnp.where(index == ids[...], 1.0, 0.0)
        gt[rows, :] = (scale * (jnp.exp(lt[rows, :] - logsum) - hot)).astype(jnp.bfloat16)


def grad_call(ids, rows, stats, lt, block):
    return pl.pallas_call(
        functools.partial(grad_kernel, block=block),
        in_specs=[INSIDE] * 4,
        out_specs=INSIDE,
        out_shape=pltpu.VMEM(lt.shape, jnp.bfloat16),
        compiler_params=params(4 * MIB),
        name="grad_logits",
    )(ids, rows, stats, lt)


def input_kernel(place, gt, *refs, base, tok, width):
    *weights, near, far, held = refs
    parity = place[1, base] & 1
    for x in range(held.shape[0]):
        cols = pl.ds(pl.multiple_of((2 * x + parity) * width, 128), width)
        total, row = None, 0
        for w in weights:
            term = lax.dot_general(
                gt[row : row + w.shape[0], :],
                w[:, cols],
                (((0,), (0,)), ((), ())),
                preferred_element_type=jnp.float32,
            )
            total, row = term if total is None else total + term, row + w.shape[0]
        held[x] = total.astype(jnp.bfloat16)
    at = base
    for out in (near, far):
        for k in range(out.shape[0]):
            row = pl.multiple_of(place[0, at] * tok, tok)
            out[k] = held[place[1, at] >> 1, pl.ds(row, tok), :]
            at += 1


def input_call(place, gt, weights, base, tok, width):
    vocab, tokens = gt.shape
    wide = weights[0].shape[1]
    pairs = wide // width // 2
    piece = jax.ShapeDtypeStruct((tokens // tok * pairs // 2, tok, width), jnp.bfloat16)
    return pl.pallas_call(
        functools.partial(input_kernel, base=base, tok=tok, width=width),
        in_specs=[SCALARS] + [INSIDE] * (1 + len(weights)),
        out_specs=[INSIDE] * 2,
        out_shape=[piece, piece],
        scratch_shapes=[pltpu.VMEM((pairs, tokens, width), jnp.bfloat16)],
        compiler_params=params(2 * MIB + 4 * tokens * vocab + 8 * tokens * width),
        cost_estimate=cost(vocab, wide // 2, tokens),
        name="input_grad",
    )(place, gt, *weights)


def weight_kernel(gt, h, *refs):
    out = refs[-1]
    out[...] = jnp.dot(gt[...], h[...], preferred_element_type=jnp.float32).astype(jnp.bfloat16)


def weight_call(gt, h, block, first, count, held=None):
    vocab, tokens = gt.shape
    wide = h.shape[1]
    specs = [pl.BlockSpec((block, tokens), lambda i: (first + i, 0)), whole((tokens, wide))]
    return pl.pallas_call(
        weight_kernel,
        grid=(count,),
        in_specs=specs + ([] if held is None else [pl.BlockSpec(memory_space=pl.ANY)]),
        out_specs=pl.BlockSpec((block, wide), lambda i: (first + i, 0)),
        out_shape=jax.ShapeDtypeStruct((vocab, wide), jnp.bfloat16),
        input_output_aliases={} if held is None else {2: 0},
        compiler_params=params(4 * block * wide + 2 * MIB),
        cost_estimate=cost(count * block, wide, tokens),
        name="weight_grad",
    )(gt, h, *([] if held is None else [held]))


def merge(a, b):
    top = jnp.maximum(a[0], b[0])
    total = a[1] * jnp.exp(a[0] - top) + b[1] * jnp.exp(b[0] - top)
    return jnp.stack([top, total, a[2] + b[2]])


def places(grid, z, x, c, y):
    shape = (2, 8 * grid.pipe)
    at = lax.broadcasted_iota(jnp.int32, shape, 1)
    dz, b1 = at % grid.pipe, at // grid.pipe % 2
    b2, core = at // (2 * grid.pipe) % 2, c ^ (at // (4 * grid.pipe))
    dx, dy = jnp.where(core == 0, b1, b2), jnp.where(core == 0, b2, b1)
    row, col = (z ^ dz) * grid.dp + (y ^ dy), 2 * (x ^ dx) + core
    return jnp.where(lax.broadcasted_iota(jnp.int32, shape, 0) == 0, row, col).astype(jnp.int32)


def after(value, *others):
    return lax.optimization_barrier((value,) + others)[0]


def gather_fast(grid, hidden, weight):
    rows = weight.shape[0] // 4
    got = [grid.send(hidden, z_swap(dz)) for dz in range(1, grid.pipe)]
    held = [load_call(weight, 0, rows)]
    *got, held[0] = lax.optimization_barrier((*got, held[0]))
    own = jnp.stack([hidden, *got])
    first = grid.send(own, first_swap)
    second = grid.send(own, second_swap)
    held += [load_call(after(weight, own), k * rows, rows) for k in (1, 2)]
    first, second, *held = lax.optimization_barrier((first, second, *held))
    both = grid.send(first, second_swap)
    held.append(load_call(after(weight, first), 3 * rows, rows))
    mine = [own, first, second, both]
    return mine + [grid.send(part, core_swap) for part in mine], held


def gather_rows(grid, value, z, y):
    tok = value.shape[1]
    parts = [value if dz == 0 else grid.send(value, z_swap(dz)) for dz in range(grid.pipe)]
    held = jnp.stack(parts)
    held = jnp.stack([held, grid.send(held, y_swap)])
    shape = (grid.dp, grid.pipe, value.shape[0], tok, tok * grid.pipe * grid.dp)
    dy, dz, item, token = (lax.broadcasted_iota(jnp.int32, shape, k) for k in (0, 1, 3, 4))
    hit = ((z ^ dz) * grid.dp + (y ^ dy)) * tok + item == token
    return jnp.sum(jnp.where(hit, held[..., None], 0.0), axis=(0, 1, 3))


def merge_kernel(a, b, out):
    top = jnp.maximum(a[0:1, :], b[0:1, :])
    out[0:1, :] = top
    out[1:2, :] = a[1:2, :] * jnp.exp(a[0:1, :] - top) + b[1:2, :] * jnp.exp(b[0:1, :] - top)
    out[2:3, :] = a[2:3, :] + b[2:3, :]


def merge_call(a, b):
    return pl.pallas_call(
        merge_kernel,
        in_specs=[INSIDE] * 2,
        out_specs=INSIDE,
        out_shape=jax.ShapeDtypeStruct(a.shape, a.dtype),
        compiler_params=params(MIB),
        name="merge_stats",
    )(a, b)


def merge_fast(grid, stats, weight):
    moves = [core_swap, x_swap, y_swap]
    k = 1
    while k < grid.pipe:
        moves.append(z_swap(k))
        k *= 2
    rows, slabs = weight.shape[0] // 4, []
    for n, move in enumerate(moves):
        got = grid.send(stats, move)
        if n >= len(moves) - 2:
            slab = load_call(after(weight, stats), (len(slabs) + 1) * rows, rows)
            got, slab = lax.optimization_barrier((got, slab))
            slabs.append(slab)
        stats = merge_call(stats, got)
    return stats, *slabs


def plus_kernel(*refs, terms):
    at = 0
    for out in refs[terms:]:
        rows = pl.ds(at, out.shape[0])
        total = refs[0][rows].astype(jnp.float32)
        for term in refs[1:terms]:
            total += term[rows].astype(jnp.float32)
        out[...] = total.astype(jnp.bfloat16)
        at += out.shape[0]


def plus(*terms, split=1):
    count = terms[0].shape[0] // split
    part = jax.ShapeDtypeStruct((count,) + terms[0].shape[1:], jnp.bfloat16)
    return pl.pallas_call(
        functools.partial(plus_kernel, terms=len(terms)),
        in_specs=[INSIDE] * len(terms),
        out_specs=[INSIDE] * split,
        out_shape=[part] * split,
        compiler_params=params(4 * MIB),
        name="add_terms",
    )(*terms)


def gradients_fast(grid, place, gt, h, weight, block, tok, width):
    blocks = gt.shape[0] // block
    cuts = [0, blocks * 4 // 8, blocks * 6 // 8, blocks]

    def weight_part(k, held, *others):
        return weight_call(after(gt, *others), h, block, cuts[k], cuts[k + 1] - cuts[k], held)

    half = grid.dp * grid.pipe * 2
    near_away, far_away = input_call(place, gt, weight, half, tok, width)
    far_got = grid.send(far_away, core_swap)
    near_got = grid.send(near_away, core_swap)
    near, far = input_call(place, after(gt, far_away), weight, 0, tok, width)
    far_got, near_got, far, near = lax.optimization_barrier((far_got, near_got, far, near))
    (far,) = plus(far, far_got)
    got = grid.send(far, second_swap)
    out = weight_part(0, None, far)
    got, near_got, out = lax.optimization_barrier((got, near_got, out))
    near, far = plus(near, near_got, got, split=2)
    got = grid.send(far, first_swap)
    out = weight_part(1, out, far)
    got, out = lax.optimization_barrier((got, out))
    near, *far = plus(near, got, split=grid.pipe)
    got = [grid.send(part, z_swap(k + 1)) for k, part in enumerate(far)]
    out = weight_part(2, out, near)
    *got, out = lax.optimization_barrier((*got, out))
    return plus(near, *got)[0][0], out


def local_fast(grid, hidden, weight, targets, loss_grad):
    tok, width = hidden.shape
    vocab = weight.shape[0]
    tokens = tok * grid.pipe * grid.dp
    z, t, y = (lax.axis_index(name) for name in AXES)
    offset = ((z * grid.tensor + t) * grid.dp + y) * vocab
    start = (z * grid.dp + y) * tok
    z, x, c, y, offset, start, weight = lax.optimization_barrier(
        (z, t >> 1, t & 1, y, offset, start, weight)
    )
    weight = pltpu.with_memory_space_constraint(weight, pltpu.HBM)
    place = places(grid, z, x, c, y)
    parts, slabs = gather_fast(grid, hidden, weight)
    rows = jnp.stack([targets.astype(jnp.float32), loss_grad.astype(jnp.float32)])
    rows = gather_rows(grid, after(rows, parts[0]), z, y)
    ids = rows[0:1].astype(jnp.int32) - offset
    h, lt, stats = logits_call(place, ids, parts, slabs, tokens, 512)
    stats, slabs[1], slabs[2] = merge_fast(grid, stats, weight)
    gt = grad_call(ids, rows, stats, lt, 512)
    input_grad, weight_grad = gradients_fast(grid, place, gt, h, slabs, 512, tok, width)
    stats = after(stats, input_grad)
    logsum = stats[0:1] + jnp.log(stats[1:2])
    shape = (tok, tokens)
    own = lax.broadcasted_iota(jnp.int32, shape, 0) + start
    own = own == lax.broadcasted_iota(jnp.int32, shape, 1)
    token_loss = jnp.sum(jnp.where(own, logsum - stats[2:3], 0.0), axis=1)
    return token_loss, weight_grad, input_grad


def local_any(grid, hidden, weight, targets, loss_grad):
    tok, vocab = hidden.shape[0], weight.shape[0]
    z, t, y = (lax.axis_index(name) for name in AXES)
    blocks = ("pipe", "dp")
    rows = lax.all_gather(hidden, "tensor", axis=1, tiled=True)
    rows = lax.all_gather(rows, blocks, axis=0, tiled=True)
    offset = ((z * grid.tensor + t) * grid.dp + y) * vocab
    ids = lax.all_gather(targets, blocks, axis=0, tiled=True) - offset
    scale = lax.all_gather(loss_grad.astype(jnp.float32), blocks, axis=0, tiled=True)
    logits = lax.dot_general(
        rows, weight, (((1,), (1,)), ((), ())), preferred_element_type=jnp.float32
    )
    hot = (lax.broadcasted_iota(jnp.int32, logits.shape, 1) == ids[:, None]).astype(jnp.float32)
    top = jnp.max(logits, axis=1)
    total = jnp.sum(jnp.exp(logits - top[:, None]), axis=1)
    every = lax.all_gather(jnp.stack([top, total, jnp.sum(logits * hot, axis=1)]), AXES, axis=0)
    stats = functools.reduce(merge, [every[i] for i in range(every.shape[0])])
    logsum = stats[0] + jnp.log(stats[1])
    token_loss = lax.dynamic_slice_in_dim(logsum - stats[2], (z * grid.dp + y) * tok, tok, 0)
    grad = (scale[:, None] * (jnp.exp(logits - logsum[:, None]) - hot)).astype(jnp.bfloat16)
    weight_grad = lax.dot_general(
        grad, rows, (((0,), (0,)), ((), ())), preferred_element_type=jnp.float32
    ).astype(jnp.bfloat16)
    term = jnp.dot(grad, weight, preferred_element_type=jnp.float32).astype(jnp.bfloat16)
    term = lax.psum_scatter(term, "tensor", scatter_dimension=1, tiled=True)
    return token_loss, weight_grad, lax.psum_scatter(term, blocks, scatter_dimension=0, tiled=True)


def local(grid, hidden, weight, targets, loss_grad):
    vocab = weight.shape[0]
    exact = grid.pipe * grid.tensor * grid.dp * vocab <= 2**24
    fast = grid.tensor == 4 and grid.dp == 2 and grid.pipe in (1, 2, 4)
    fast = fast and exact and hidden.shape[1] % 128 == 0 and vocab % 4096 == 0
    body = local_fast if fast else local_any
    return body(grid, hidden, weight, targets, loss_grad)


def solution(mesh):
    in_specs = (
        P(("pipe", "dp"), "tensor"),
        P(("pipe", "tensor", "dp"), None),
        P(("pipe", "dp")),
        P(("pipe", "dp")),
    )
    out_specs = (P(("pipe", "dp")), P(("pipe", "tensor", "dp"), None), P(("pipe", "dp"), "tensor"))
    grid = Grid(tuple(mesh.shape[name] for name in AXES))
    return jax.shard_map(
        functools.partial(local, grid),
        mesh=mesh,
        in_specs=in_specs,
        out_specs=out_specs,
        check_vma=False,
    )
```
